32 devices in a mesh: seq: 8 (over z, y), tensor: 4 (over x, core).
Axes of the slice: x: 2, y: 2, z: 4, core: 2. Of those that a mesh axis runs over, the one named last changes fastest.
Arguments:
- queries: bfloat16 [2048, 8192], P('seq', 'tensor'), may hold values from -4 to 4, as said below
- keys: bfloat16 [2048, 1024], P('seq', 'tensor'), may hold values from -96 to 96, as said below
- values: bfloat16 [2048, 1024], P('seq', 'tensor'), may hold values from -6 to 6
- block_pos: int32 [16], replicated, may hold values from 0 to 15, each once
Outputs:
- attended: bfloat16 [2048, 8192], P('seq')
The draws below stay inside these ranges and needn't reach their ends.
Inputs may be any that keep to these rules, and one draw needn't show every extreme that they name: block_pos is a permutation of 0 to 15. real-valued queries. real-valued keys.
All inputs are finite; a program needn't handle non-finite values.
Results may differ from the reference program's by a relative error of at most 0.004.
Values may be sent and summed in bfloat16 or wider, within the bound.
A program may use at most 64 MiB of HBM per device.

```python
import math
import jax
import jax.numpy as jnp
from jax import lax

QUERY_HEADS = 64
KEY_VALUE_HEADS = 8
HEAD_WIDTH = 128
VISIBLE_SHARDS = 4
SHARD_TOKENS = 256
BLK = 128
NB = 16
SEQUENCE_TOKENS = 2048
N_SEQ = 8


def shared_fields(key):
    base = jax.random.fold_in(key, 7)
    key_q, key_sample = jax.random.split(base, 2)
    query_field = jnp.clip(jax.random.normal(key_q, (SEQUENCE_TOKENS, QUERY_HEADS * HEAD_WIDTH), jnp.float32), -4.0, 4.0)
    key_tensor = jnp.clip(jax.random.normal(key_sample, (SEQUENCE_TOKENS, KEY_VALUE_HEADS * HEAD_WIDTH), jnp.float32), -4.0, 4.0)
    return (query_field, key_tensor)


def draw_queries(key, part):
    return shared_fields(key)[0].astype(jnp.bfloat16)


def draw_keys(key, part):
    return shared_fields(key)[1].astype(jnp.bfloat16)


def block_scale(stream_key, extent, pieces, smallest, top_value):
    loudness, own = 1.0, jax.random.fold_in(stream_key, 6)
    for dim, parts in pieces:
        steps = jnp.exp(jax.random.uniform(jax.random.fold_in(own, dim), (parts,), jnp.float32, smallest / len(pieces), top_value / len(pieces)))
        loudness = loudness * jnp.repeat(steps, extent[dim] // parts).reshape([-1 if axis == dim else 1 for axis in range(len(extent))])
    return loudness


def scatter_about(own_key, extent, width, bound, cuts=(), kind=jnp.bfloat16):
    array = jax.random.normal(own_key, extent, jnp.float32) * width
    if len(cuts) > 0:
        array = block_scale(own_key, extent, cuts, -0.22, 0.18) * array
    return jnp.clip(array, min=-bound, max=bound).astype(kind)


def setup_inputs(seed: int = 0) -> dict:
    seeds = jax.random.split(jax.random.key(seed), 5)
    queries = draw_queries(jax.random.fold_in(seeds[4], 71), 0)
    keys = draw_keys(jax.random.fold_in(seeds[4], 71), 0)
    values = scatter_about(seeds[2], (SEQUENCE_TOKENS, KEY_VALUE_HEADS * HEAD_WIDTH), 1.0, 6.0, ((0, 8), (1, 4)))
    block_pos = jax.random.permutation(seeds[3], NB).astype(jnp.int32)
    return dict(queries=queries, keys=keys, values=values, block_pos=block_pos)


def reference(queries, keys, values, block_pos):
    group_factor = QUERY_HEADS // KEY_VALUE_HEADS
    scale = 1.0 / math.sqrt(HEAD_WIDTH)
    offsets = jnp.arange(BLK, dtype=jnp.int32)
    positions = (block_pos[:, None].astype(jnp.int32) * BLK + offsets[None, :]).reshape(-1)

    def one_shard(shard):
        start = (shard * SHARD_TOKENS).astype(jnp.int32)
        query_rows = lax.dynamic_slice_in_dim(queries, start, SHARD_TOKENS, 0).astype(jnp.float32)
        query_rows = query_rows.reshape(SHARD_TOKENS, KEY_VALUE_HEADS, group_factor, HEAD_WIDTH)
        q_pos = lax.dynamic_slice_in_dim(positions, start, SHARD_TOKENS, 0)
        key_collection = []
        value_collection = []
        pos_list = []
        for back in range(VISIBLE_SHARDS):
            source = ((shard - back) % N_SEQ * SHARD_TOKENS).astype(jnp.int32)
            key_collection.append(lax.dynamic_slice_in_dim(keys, source, SHARD_TOKENS, 0))
            value_collection.append(lax.dynamic_slice_in_dim(values, source, SHARD_TOKENS, 0))
            pos_list.append(lax.dynamic_slice_in_dim(positions, source, SHARD_TOKENS, 0))
        key_gathered = jnp.concatenate(key_collection, 0).astype(jnp.float32).reshape(VISIBLE_SHARDS * SHARD_TOKENS, KEY_VALUE_HEADS, HEAD_WIDTH)
        value_gathered = jnp.concatenate(value_collection, 0).astype(jnp.float32).reshape(VISIBLE_SHARDS * SHARD_TOKENS, KEY_VALUE_HEADS, HEAD_WIDTH)
        key_pos = jnp.concatenate(pos_list, 0)
        scores = jnp.einsum('qgrd,kgd->grqk', query_rows, key_gathered) * scale
        allowed = key_pos[None, :] <= q_pos[:, None]
        scores = jnp.where(allowed[None, None], scores, -1e+30)
        top = lax.optimization_barrier(jnp.max(scores, axis=-1, keepdims=True))
        weights = jnp.exp(scores - top)
        total = lax.optimization_barrier(jnp.sum(weights, axis=-1))
        rounded = lax.optimization_barrier(weights.astype(jnp.bfloat16)).astype(jnp.float32)
        mixed = jnp.einsum('grqk,kgd->qgrd', rounded, value_gathered)
        mixed = mixed / jnp.transpose(total, (2, 0, 1))[..., None]
        return mixed.reshape(SHARD_TOKENS, QUERY_HEADS * HEAD_WIDTH).astype(jnp.bfloat16)
    shards = lax.map(one_shard, jnp.arange(N_SEQ, dtype=jnp.int32))
    return shards.reshape(SEQUENCE_TOKENS, QUERY_HEADS * HEAD_WIDTH)
```

```python
import functools
import math

import jax
import jax.numpy as jnp
from jax import lax
from jax.experimental import pallas as pl
from jax.experimental.pallas import tpu as pltpu
from jax.sharding import PartitionSpec as P

HEAD = 128
GROUP = 8
CUTS = 2
PIECES = 2 * CUTS
WINDOW = 4
SHARE = 5
CROSS = (0, 1)
BESIDE = (0, 1, 2)
MESH = pl.DeviceIdType.MESH


def kernel(n, T, rows, groups, share, q_hbm, k_hbm, v_hbm, bp_hbm, out, bp, qv, qx, kv, bias,
           ld_sem, kv_send, kv_recv, xk_send, xk_recv, x_send, x_recv, c_send, c_recv):
    s = lax.axis_index("seq")
    t = lax.axis_index("tensor")
    heads = groups * GROUP
    solo = heads - share
    last = groups - 1
    hops = T // 2 - 1
    half = rows // 2
    cut = rows // CUTS

    def seq_dev(d):
        return (lax.rem(s + d + n, n), t)

    def x_dev(k):
        return (s, lax.rem(t + 2 * k + T, T))

    sibling = (s, t + 1 - 2 * lax.rem(t, 2))
    partner = lax.rem(t + 2, T)
    odd = lax.rem(s, 2)

    loads = []
    for g in range(groups):
        cols = pl.ds(g * HEAD, HEAD)
        pair = []
        for i, src in enumerate((k_hbm, v_hbm)):
            c = pltpu.make_async_copy(src.at[:, cols], kv.at[g, 0, i], ld_sem.at[g, i])
            c.start()
            pair.append(c)
        loads.append(pair)
    q_parts = []
    for i, (lo, hi) in enumerate(((solo, heads), (0, solo))):
        if hi > lo:
            cols = pl.ds(lo * HEAD, (hi - lo) * HEAD)
            c = pltpu.make_async_copy(q_hbm.at[:, cols], qv.at[:, cols], ld_sem.at[groups, i])
            c.start()
            q_parts.append(c)
    bp_load = pltpu.make_async_copy(bp_hbm, bp, ld_sem.at[groups + 1, 0])
    bp_load.start()

    barrier = pltpu.get_barrier_semaphore()

    def greet(p):
        pl.semaphore_signal(barrier, inc=1, device_id=p, device_id_type=MESH)

    near = [sibling] + [x_dev(k) for k in range(1, hops + 1)]
    for p in near:
        greet(p)

    @pl.when(odd == 0)
    def _():
        for d in (1, -2, -1):
            greet(seq_dev(d))
        pl.semaphore_wait(barrier, len(near) + 2)

    @pl.when(odd == 1)
    def _():
        for d in (-1, -2):
            greet(seq_dev(d))
        pl.semaphore_wait(barrier, len(near) + 3)

    def kv_copy(g, i, b, src, d, sent):
        part = pl.ds(i % CUTS * cut, cut)
        return pltpu.make_async_remote_copy(
            src_ref=kv.at[g, src, i // CUTS, part], dst_ref=kv.at[g, b, i // CUTS, part],
            send_sem=kv_send.at[g, i, sent], recv_sem=kv_recv.at[g, i, b - 1],
            device_id=seq_dev(d), device_id_type=MESH)

    def got(g, i, b):
        kv_copy(g, i, b, 0, 1, 0).wait_recv()

    def send_own(g, i):
        kv_copy(g, i, 2, 0, 2, 1).start()

        @pl.when(odd == 0)
        def _():
            kv_copy(g, i, 1, 0, 1, 0).start()

    def relay_two(g):
        for i in range(PIECES):
            got(g, i, 2)

            @pl.when(odd == 1)
            def _():
                kv_copy(g, i, 1, 2, -1, 0).start()
                if i in CROSS:
                    kv_copy(g, i, 3, 2, 1, 2).start()

            if i in BESIDE:
                @pl.when(odd == 0)
                def _():
                    kv_copy(g, i, 3, 2, 1, 2).start()

    def relay_one(g):
        for i in range(PIECES):
            got(g, i, 1)
            if i not in BESIDE:
                @pl.when(odd == 1)
                def _():
                    kv_copy(g, i, 3, 1, 2, 3).start()
            if i not in CROSS:
                @pl.when(odd == 0)
                def _():
                    kv_copy(g, i, 3, 1, 2, 3).start()

    def xk_copy(i):
        return pltpu.make_async_remote_copy(
            src_ref=kv.at[last, 0, i], dst_ref=kv.at[groups, 0, i],
            send_sem=xk_send.at[i], recv_sem=xk_recv.at[i],
            device_id=x_dev(1), device_id_type=MESH)

    def xq_copy():
        return pltpu.make_async_remote_copy(
            src_ref=qv.at[:, pl.ds(solo * HEAD, share * HEAD)], dst_ref=qx,
            send_sem=xk_send.at[2], recv_sem=xk_recv.at[2],
            device_id=x_dev(1), device_id_type=MESH)

    for i in range(PIECES):
        if i % CUTS == 0:
            loads[0][i // CUTS].wait()
        send_own(0, i)
    for g in range(1, groups):
        for i in range(PIECES):
            if i % CUTS == 0:
                loads[g][i // CUTS].wait()
                if share and g == last:
                    xk_copy(i // CUTS).start()
            send_own(g, i)
    for c in q_parts:
        c.wait()
        if share and c is q_parts[0]:
            xq_copy().start()

    bp_load.wait()
    blk = half
    lane = lax.broadcasted_iota(jnp.int32, (blk, blk), 1)
    sub = lax.broadcasted_iota(jnp.int32, (blk, blk), 0)
    for i in range(2):
        qpos = bp[2 * s + i] * blk + sub
        for b in range(WINDOW):
            owner = lax.rem(s - b + n, n)
            for j in range(2):
                kpos = bp[2 * owner + j] * blk + lane
                bias[i * blk:(i + 1) * blk, (2 * b + j) * blk:(2 * b + j + 1) * blk] = (
                    jnp.where(kpos <= qpos, 0.0, -1e30).astype(jnp.float32))

    relay_two(0)
    relay_one(0)
    if share:
        for i in range(PIECES):
            if i % CUTS == 0:
                xk_copy(i // CUTS).wait_recv()
            send_own(groups, i)

    def piece(owner, h):
        col = pl.multiple_of((owner * heads + h) * HEAD, HEAD)
        return out.at[:, pl.ds(col, HEAD)]

    def x_copy(k, h, owner):
        return pltpu.make_async_remote_copy(
            src_ref=piece(owner, h), dst_ref=piece(owner, h),
            send_sem=x_send.at[k - 1, h], recv_sem=x_recv.at[k - 1, h],
            device_id=x_dev(k), device_id_type=MESH)

    def c_copy(k, h, owner):
        return pltpu.make_async_remote_copy(
            src_ref=piece(owner, h), dst_ref=piece(owner, h),
            send_sem=c_send.at[k, h], recv_sem=c_recv.at[k, h],
            device_id=sibling, device_id_type=MESH)

    factor = math.log2(math.e) / math.sqrt(HEAD)
    window = WINDOW * rows

    def attend(g, queries, qcol, owner, h):
        qcol = pl.multiple_of(qcol, HEAD)
        ocol = pl.multiple_of((owner * heads + h) * HEAD, HEAD)
        keys = kv[g, :, 0].reshape(window, HEAD)
        made = []
        for i in range(2):
            part = slice(i * half, (i + 1) * half)
            q = queries[part, pl.ds(qcol, HEAD)]
            sc = lax.dot_general(q, keys, (((1,), (1,)), ((), ())),
                                 preferred_element_type=jnp.float32)
            sc = sc + bias[part, :]
            top = jnp.max(sc, axis=1, keepdims=True)
            w = jnp.exp2((sc - top) * factor)
            total = jnp.sum(w, axis=1, keepdims=True)
            made.append((part, w.astype(jnp.bfloat16), total))
        vals = kv[g, :, 1].reshape(window, HEAD)
        for part, w, total in made:
            mixed = jnp.dot(w, vals, preferred_element_type=jnp.float32)
            out[part, pl.ds(ocol, HEAD)] = (mixed / total).astype(out.dtype)

    def own_head(h, _, g):
        attend(g, qv, h * HEAD, t, h)

        @pl.when(h < solo)
        def _():
            for k in range(1, hops + 1):
                x_copy(k, h, t).start()

        c_copy(0, h, t).start()
        return 0

    def partner_head(r, _):
        attend(groups, qx, r * HEAD, partner, solo + r)
        c_copy(1, solo + r, partner).start()
        return 0

    def forward(h, _):
        for k in range(1, hops + 1):
            owner = lax.rem(t - 2 * k + T, T)
            x_copy(k, h, owner).wait_recv()
            c_copy(k, h, owner).start()
        return 0

    total_groups = groups + (1 if share else 0)
    for g in range(groups):
        for i in range(PIECES):
            got(g, i, 3)
        base = g * GROUP
        body = functools.partial(own_head, g=g)
        more = g + 1 < total_groups
        lax.fori_loop(base, base + 2, body, 0)
        if more:
            relay_two(g + 1)
        lax.fori_loop(base + 2, base + 4, body, 0)
        if more:
            relay_one(g + 1)
        lax.fori_loop(base + 4, base + GROUP, body, 0)

    early = solo // 2
    lax.fori_loop(0, early, forward, 0)
    if share:
        for i in range(PIECES):
            got(groups, i, 3)
        xq_copy().wait_recv()
        lax.fori_loop(0, share, partner_head, 0)
    lax.fori_loop(early, solo, forward, 0)

    def finish(h, _):
        for k in range(hops + 1):
            c_copy(k, h, t).wait()

        @pl.when(h < solo)
        def _():
            for k in range(1, hops + 1):
                x_copy(k, h, t).wait_send()

        return 0

    lax.fori_loop(0, heads, finish, 0)
    if share:
        for i in range(2):
            xk_copy(i).wait_send()
        xq_copy().wait_send()
    for g in range(total_groups):
        for i in range(PIECES):
            kv_copy(g, i, 1, 0, 1, 0).wait_send()
            kv_copy(g, i, 2, 0, 2, 1).wait_send()
            for parity, sent, when in ((1, 2, i in CROSS), (0, 2, i in BESIDE),
                                       (1, 3, i not in BESIDE), (0, 3, i not in CROSS)):
                if when:
                    @pl.when(odd == parity)
                    def _():
                        kv_copy(g, i, 3, 0, 1, sent).wait_send()


def body(n, T, queries, keys, values, block_pos):
    rows = queries.shape[0]
    groups = keys.shape[1] // HEAD
    heads = groups * GROUP
    hops = T // 2 - 1
    share = SHARE if hops == 1 and groups > 1 else 0
    total = groups + (1 if share else 0)
    dma = pltpu.SemaphoreType.DMA
    return pl.pallas_call(
        functools.partial(kernel, n, T, rows, groups, share),
        out_shape=jax.ShapeDtypeStruct((rows, queries.shape[1] * T), jnp.bfloat16),
        in_specs=[pl.BlockSpec(memory_space=pltpu.HBM)] * 4,
        out_specs=pl.BlockSpec(memory_space=pltpu.VMEM),
        scratch_shapes=[
            pltpu.SMEM(block_pos.shape, jnp.int32),
            pltpu.VMEM((rows, heads * HEAD), jnp.bfloat16),
            pltpu.VMEM((rows, max(share, 1) * HEAD), jnp.bfloat16),
            pltpu.VMEM((total, WINDOW, 2, rows, HEAD), jnp.bfloat16),
            pltpu.VMEM((rows, WINDOW * rows), jnp.float32),
            dma((groups + 2, 2)),
            dma((total, PIECES, 4)),
            dma((total, PIECES, 3)),
            dma((3,)),
            dma((3,)),
            dma((hops, heads)),
            dma((hops, heads)),
            dma((hops + 1, heads)),
            dma((hops + 1, heads)),
        ],
        compiler_params=pltpu.CompilerParams(
            collective_id=0, has_side_effects=True, vmem_limit_bytes=32 * 1024 * 1024),
    )(*(pltpu.with_memory_space_constraint(z, pltpu.HBM)
        for z in (queries, keys, values, block_pos)))


def solution(mesh):
    n, T = mesh.shape["seq"], mesh.shape["tensor"]
    placed = (P("seq", "tensor"), P("seq", "tensor"), P("seq", "tensor"), P())
    return jax.shard_map(functools.partial(body, n, T), mesh=mesh, in_specs=placed,
                         out_specs=P("seq", None), check_vma=False)
```

```python
import functools
import math

import jax
import jax.numpy as jnp
from jax import lax
from jax.experimental import pallas as pl
from jax.experimental.pallas import tpu as pltpu
from jax.sharding import PartitionSpec as P

HEAD = 128
GROUP = 8
CUTS = 2
PIECES = 2 * CUTS
WINDOW = 4
SHARE = (8, 0)
AHEAD = (6, 10)
CROSS = ((0, 1, 2, 3), (0, 1), (0, 1))
BESIDE = ((0, 1, 2, 3), (0, 1, 2, 3), (0, 1, 2, 3))
MESH = pl.DeviceIdType.MESH


def kernel(n, T, rows, groups, share, q_hbm, k_hbm, v_hbm, bp_hbm, out, bp, qv, qx, kv, bias,
           ld_sem, go_sem, own_send, relay_send, two_recv, kind_recv, lend_send, lend_recv,
           x_send, x_recv, c_send, c_recv):
    s = lax.axis_index("seq")
    t = lax.axis_index("tensor")
    core = lax.rem(t, 2)
    heads = groups * GROUP
    keep = tuple(heads - m for m in share)
    last = groups - 1
    every = groups + (1 if any(share) else 0)
    hops = T // 2 - 1
    half = rows // 2
    cut = rows // CUTS

    def cross(g):
        return CROSS[min(g, 2)]

    def beside(g):
        return BESIDE[min(g, 2)]

    def seq_dev(d):
        return (lax.rem(s + d + n, n), t)

    def x_dev(k):
        return (s, lax.rem(t + 2 * k + T, T))

    sibling = (s, t + 1 - 2 * core)
    other = lax.rem(t + 3 - 2 * core, T)
    match = (s, other)
    odd = lax.rem(s, 2)

    def on_core(c):
        return pl.when(core == c)

    def lenders(f):
        for c in range(2):
            if share[c]:
                on_core(c)(functools.partial(f, share[c], keep[c]))

    def borrowers(f):
        for c in range(2):
            if share[c]:
                on_core(1 - c)(functools.partial(f, share[c], keep[c]))

    for g in range(groups):
        cols = pl.ds(g * HEAD, HEAD)
        for i, src in enumerate((k_hbm, v_hbm)):
            pltpu.make_async_copy(src.at[:, cols], kv.at[g, 0, i], ld_sem.at[min(g, 1)]).start()
    q_load = pltpu.make_async_copy(q_hbm, qv, ld_sem.at[2])
    q_load.start()
    bp_load = pltpu.make_async_copy(bp_hbm, bp, ld_sem.at[3])
    bp_load.start()

    barrier = pltpu.get_barrier_semaphore()

    def greet(p):
        pl.semaphore_signal(barrier, inc=1, device_id=p, device_id_type=MESH)

    near = [sibling] + [x_dev(k) for k in range(1, hops + 1)]
    for p in near:
        greet(p)
    borrowers(lambda m, first: greet(match))

    @pl.when(odd == 0)
    def _():
        for d in (1, -2, -1):
            greet(seq_dev(d))

    @pl.when(odd == 1)
    def _():
        for d in (-1, -2):
            greet(seq_dev(d))

    for c in range(2):
        @on_core(c)
        def _():
            pl.semaphore_wait(barrier, len(near) + 2 + (1 if share[c] else 0) + odd)

    def kv_copy(g, i, b, src, d, own=False):
        part = pl.ds(i % CUTS * cut, cut)
        return pltpu.make_async_remote_copy(
            src_ref=kv.at[g, src, i // CUTS, part], dst_ref=kv.at[g, b, i // CUTS, part],
            send_sem=(own_send if own else relay_send).at[g],
            recv_sem=two_recv.at[g, i] if b == 2 else kind_recv.at[g, b // 2, i // CUTS],
            device_id=seq_dev(d), device_id_type=MESH)

    def slots(g, ref, sem):
        return pltpu.make_async_remote_copy(
            src_ref=ref, dst_ref=ref, send_sem=sem, recv_sem=sem,
            device_id=sibling, device_id_type=MESH)

    def got(g, b, kind):
        slots(g, kv.at[g, b, kind], kind_recv.at[g, b // 2, kind]).wait_recv()

    def send_own(g):
        for i in range(PIECES):
            kv_copy(g, i, 2, 0, 2, True).start()

            @pl.when(odd == 0)
            def _():
                kv_copy(g, i, 1, 0, 1, True).start()

    def relay_two(g):
        for i in range(PIECES):
            kv_copy(g, i, 2, 0, 2).wait_recv()

            @pl.when(odd == 1)
            def _():
                kv_copy(g, i, 1, 2, -1).start()
                if i in cross(g):
                    kv_copy(g, i, 3, 2, 1).start()

            if i in beside(g):
                @pl.when(odd == 0)
                def _():
                    kv_copy(g, i, 3, 2, 1).start()

    def relay_one(g, kind):
        got(g, 1, kind)
        for i in range(kind * CUTS, (kind + 1) * CUTS):
            if i not in beside(g):
                @pl.when(odd == 1)
                def _():
                    kv_copy(g, i, 3, 1, 2).start()
            if i not in cross(g):
                @pl.when(odd == 0)
                def _():
                    kv_copy(g, i, 3, 1, 2).start()

    def own_sent(g):
        for parity, count in ((0, 2), (1, 1)):
            @pl.when(odd == parity)
            def _():
                slots(g, kv.at[g, 0:count], own_send.at[g]).wait_send()

    def relays_sent(g):
        ways = len(beside(g)) - len(cross(g))
        for parity, count in ((0, PIECES + ways), (1, 2 * PIECES - ways)):
            @pl.when(odd == parity)
            def _():
                slots(g, kv.at[g, 0:count // 2, 0], relay_send.at[g]).wait_send()

    def keys_lent():
        return pltpu.make_async_remote_copy(
            src_ref=kv.at[last, 0], dst_ref=kv.at[groups, 0],
            send_sem=lend_send.at[0], recv_sem=lend_recv.at[0],
            device_id=match, device_id_type=MESH)

    def queries_lent(m, first):
        return pltpu.make_async_remote_copy(
            src_ref=qv.at[:, pl.ds(first * HEAD, m * HEAD)], dst_ref=qx.at[:, pl.ds(0, m * HEAD)],
            send_sem=lend_send.at[1], recv_sem=lend_recv.at[1],
            device_id=match, device_id_type=MESH)

    def loaded(g):
        pltpu.make_async_copy(kv.at[g, 1], kv.at[g, 0], ld_sem.at[min(g, 1)]).wait()

    loaded(0)

    @on_core(1)
    def _():
        send_own(0)

    if groups > 1:
        ref = kv.at[1:groups, 0]
        pltpu.make_async_copy(ref, ref, ld_sem.at[1]).wait()
    q_load.wait()

    def lend(m, first):
        keys_lent().start()
        queries_lent(m, first).start()

    lenders(lend)

    @on_core(1)
    def _():
        own_sent(0)
        pl.semaphore_signal(go_sem, inc=1, device_id=sibling, device_id_type=MESH)

    @on_core(0)
    def _():
        pl.semaphore_wait(go_sem, 1)
        send_own(0)

    bp_load.wait()
    blk = half
    lane = lax.broadcasted_iota(jnp.int32, (blk, blk), 1)
    sub = lax.broadcasted_iota(jnp.int32, (blk, blk), 0)
    for i in range(2):
        qpos = bp[2 * s + i] * blk + sub
        for b in range(WINDOW):
            owner = lax.rem(s - b + n, n)
            for j in range(2):
                kpos = bp[2 * owner + j] * blk + lane
                bias[i * blk:(i + 1) * blk, (2 * b + j) * blk:(2 * b + j + 1) * blk] = (
                    jnp.where(kpos <= qpos, 0.0, -1e30).astype(jnp.float32))

    relay_two(0)
    for g in range(1, groups):
        send_own(g)

    def pass_on(m, first):
        keys_lent().wait_recv()
        send_own(groups)

    borrowers(pass_on)

    def piece(owner, h, count=1):
        col = pl.multiple_of((owner * heads + h) * HEAD, HEAD)
        return out.at[:, pl.ds(col, count * HEAD)]

    def x_copy(k, h, owner, count=1):
        return pltpu.make_async_remote_copy(
            src_ref=piece(owner, h, count), dst_ref=piece(owner, h, count),
            send_sem=x_send.at[k - 1], recv_sem=x_recv.at[k - 1, h // 2],
            device_id=x_dev(k), device_id_type=MESH)

    def c_copy(k, h, owner, count=1):
        return pltpu.make_async_remote_copy(
            src_ref=piece(owner, h, count), dst_ref=piece(owner, h, count),
            send_sem=c_send.at[k], recv_sem=c_recv.at[k],
            device_id=sibling, device_id_type=MESH)

    factor = math.log2(math.e) / math.sqrt(HEAD)
    window = WINDOW * rows

    def attend(g, jobs, late=None):
        keys = kv[g, :, 0].reshape(window, HEAD)
        made = []
        for queries, qcol, col in jobs:
            qcol = pl.multiple_of(qcol, HEAD)
            col = pl.multiple_of(col, HEAD)
            for i in range(2):
                part = slice(i * half, (i + 1) * half)
                q = queries[part, pl.ds(qcol, HEAD)]
                sc = lax.dot_general(q, keys, (((1,), (1,)), ((), ())),
                                     preferred_element_type=jnp.float32)
                sc = sc + bias[part, :]
                top = jnp.max(sc, axis=1, keepdims=True)
                w = jnp.exp2((sc - top) * factor)
                total = jnp.sum(w, axis=1, keepdims=True)
                made.append((part, col, w.astype(jnp.bfloat16), total))
        if late is not None:
            late()
        vals = kv[g, :, 1].reshape(window, HEAD)
        for part, col, w, total in made:
            mixed = jnp.dot(w, vals, preferred_element_type=jnp.float32)
            out[part, pl.ds(col, HEAD)] = (mixed / total).astype(out.dtype)

    def own_heads(g, first, count, late=None):
        attend(g, [(qv, h * HEAD, (t * heads + h) * HEAD) for h in range(first, first + count)], late)
        for h in range(first, first + count, 2):
            for c in range(2):
                if h < keep[c]:
                    @on_core(c)
                    def _():
                        for k in range(1, hops + 1):
                            x_copy(k, h, t, 2).start()
        c_copy(0, first, t, count).start()

    def lent_heads(r, _, step, first):
        r = r * step
        attend(groups, [(qx, (r + j) * HEAD, (other * heads + first + r + j) * HEAD) for j in range(step)])
        c_copy(hops + 1, first + r, other, step).start()
        return 0

    def forward(h, _):
        h = 2 * h
        for k in range(1, hops + 1):
            owner = lax.rem(t - 2 * k + T, T)
            x_copy(k, h, owner, 2).wait_recv()
            c_copy(k, h, owner, 2).start()
        return 0

    def relay(g, f):
        if g < groups:
            f(g)
        elif g < every:
            borrowers(lambda m, first: f(g))

    def first_relays(g):
        relay_one(g, 0)
        relay_one(g, 1)

    def arrive(g):
        got(g, 3, 0)
        got(g, 3, 1)

    def late():
        relay_one(0, 1)
        got(0, 3, 1)

    for g in range(groups):
        base = g * GROUP
        if g == 0:
            relay_one(0, 0)
            got(0, 3, 0)
            own_heads(0, 0, 2, late)
            own_heads(0, 2, 2)
        else:
            arrive(g)
            own_heads(g, base, 4)
        relay(g + 1, relay_two)
        own_heads(g, base + 4, 4)
        relay(g + 1, first_relays)

    def forwards(first, end):
        lax.fori_loop(first // 2, end // 2, forward, 0)

    done = [0, 0]

    def borrowed(m, first):
        c = 1 - share.index(m)
        stops = [min(x, keep[c]) for x in AHEAD]
        forwards(0, stops[0])
        arrive(groups)
        queries_lent(m, first).wait_recv()
        step = math.gcd(m, 4)
        for r in range(m // step):
            lent_heads(r, 0, step, first)
            if r == 0:
                forwards(stops[0], stops[1])
        done[c] = stops[1]

    borrowers(borrowed)
    for c in range(2):
        @on_core(c)
        def _():
            forwards(done[c], keep[c])

    for g in range(groups):
        relays_sent(g)
        if g > 0:
            own_sent(g)
    on_core(0)(lambda: own_sent(0))

    def settle(m, first):
        relays_sent(groups)
        own_sent(groups)
        c_copy(hops + 1, first, other, m).wait_send()

    borrowers(settle)

    def settle_lent(m, first):
        keys_lent().wait_send()
        queries_lent(m, first).wait_send()
        c_copy(hops + 1, first, t, m).wait_recv()

    lenders(settle_lent)
    c_copy(0, 0, t, heads).wait()

    for c in range(2):
        @on_core(c)
        def _():
            for k in range(1, hops + 1):
                x_copy(k, 0, t, keep[c]).wait_send()
                c_copy(k, 0, t, keep[c]).wait_send()
                c_copy(k, 0, t, keep[1 - c]).wait_recv()


def body(n, T, queries, keys, values, block_pos):
    rows = queries.shape[0]
    groups = keys.shape[1] // HEAD
    heads = groups * GROUP
    hops = T // 2 - 1
    share = SHARE if hops == 1 and groups > 1 else (0, 0)
    every = groups + (1 if any(share) else 0)
    dma = pltpu.SemaphoreType.DMA
    return pl.pallas_call(
        functools.partial(kernel, n, T, rows, groups, share),
        out_shape=jax.ShapeDtypeStruct((rows, queries.shape[1] * T), jnp.bfloat16),
        in_specs=[pl.BlockSpec(memory_space=pltpu.HBM)] * 4,
        out_specs=pl.BlockSpec(memory_space=pltpu.VMEM),
        scratch_shapes=[
            pltpu.SMEM(block_pos.shape, jnp.int32),
            pltpu.VMEM((rows, heads * HEAD), jnp.bfloat16),
            pltpu.VMEM((rows, max(*share, 1) * HEAD), jnp.bfloat16),
            pltpu.VMEM((every, WINDOW, 2, rows, HEAD), jnp.bfloat16),
            pltpu.VMEM((rows, WINDOW * rows), jnp.float32),
            dma((4,)),
            pltpu.SemaphoreType.REGULAR,
            dma((every,)),
            dma((every,)),
            dma((every, PIECES)),
            dma((every, 2, 2)),
            dma((2,)),
            dma((2,)),
            dma((hops,)),
            dma((hops, heads // 2)),
            dma((hops + 2,)),
            dma((hops + 2,)),
        ],
        compiler_params=pltpu.CompilerParams(
            collective_id=0, has_side_effects=True, vmem_limit_bytes=32 * 1024 * 1024),
    )(*(pltpu.with_memory_space_constraint(z, pltpu.HBM)
        for z in (queries, keys, values, block_pos)))


def solution(mesh):
    n, T = mesh.shape["seq"], mesh.shape["tensor"]
    placed = (P("seq", "tensor"), P("seq", "tensor"), P("seq", "tensor"), P())
    return jax.shard_map(functools.partial(body, n, T), mesh=mesh, in_specs=placed,
                         out_specs=P("seq", None), check_vma=False)
```

```python
import functools
import math

import jax
import jax.numpy as jnp
from jax import lax
from jax.experimental import pallas as pl
from jax.experimental.pallas import tpu as pltpu
from jax.sharding import PartitionSpec as P

HEAD = 128
GROUP = 8
CUTS = 2
PIECES = 2 * CUTS
WINDOW = 4
SHARE = (8, 0)
AHEAD = (6, 10)
MESH = pl.DeviceIdType.MESH


def kernel(n, T, rows, groups, share, q_hbm, k_hbm, v_hbm, bp_hbm, out, bp, qv, qx, kv, bias,
           ld_sem, go_sem, own_send, relay_send, two_recv, kind_recv, lend_send, lend_recv,
           x_send, x_recv, c_send, c_recv):
    s = lax.axis_index("seq")
    t = lax.axis_index("tensor")
    core = lax.rem(t, 2)
    heads = groups * GROUP
    keep = tuple(heads - m for m in share)
    last = groups - 1
    every = groups + (1 if any(share) else 0)
    hops = T // 2 - 1
    half = rows // 2
    cut = rows // CUTS

    def seq_dev(d):
        return (lax.rem(s + d + n, n), t)

    def x_dev(k):
        return (s, lax.rem(t + 2 * k + T, T))

    sibling = (s, t + 1 - 2 * core)
    other = lax.rem(t + 3 - 2 * core, T)
    match = (s, other)
    odd = lax.rem(s, 2)

    def on_core(c):
        return pl.when(core == c)

    def lenders(f):
        for c in range(2):
            if share[c]:
                on_core(c)(functools.partial(f, share[c], keep[c]))

    def borrowers(f):
        for c in range(2):
            if share[c]:
                on_core(1 - c)(functools.partial(f, share[c], keep[c]))

    for g in range(groups):
        cols = pl.ds(g * HEAD, HEAD)
        for i, src in enumerate((k_hbm, v_hbm)):
            pltpu.make_async_copy(src.at[:, cols], kv.at[g, 0, i], ld_sem.at[min(g, 1)]).start()
    q_load = pltpu.make_async_copy(q_hbm, qv, ld_sem.at[2])
    q_load.start()
    bp_load = pltpu.make_async_copy(bp_hbm, bp, ld_sem.at[3])
    bp_load.start()

    barrier = pltpu.get_barrier_semaphore()

    def greet(p):
        pl.semaphore_signal(barrier, inc=1, device_id=p, device_id_type=MESH)

    near = [sibling] + [x_dev(k) for k in range(1, hops + 1)]
    for p in near:
        greet(p)
    borrowers(lambda m, first: greet(match))

    @pl.when(odd == 0)
    def _():
        for d in (1, -2, -1):
            greet(seq_dev(d))

    @pl.when(odd == 1)
    def _():
        for d in (-1, -2):
            greet(seq_dev(d))

    for c in range(2):
        @on_core(c)
        def _():
            pl.semaphore_wait(barrier, len(near) + 2 + (1 if share[c] else 0) + odd)

    def kv_copy(g, i, b, src, d, own=False):
        part = pl.ds(i % CUTS * cut, cut)
        return pltpu.make_async_remote_copy(
            src_ref=kv.at[g, src, i // CUTS, part], dst_ref=kv.at[g, b, i // CUTS, part],
            send_sem=(own_send if own else relay_send).at[g],
            recv_sem=two_recv.at[g, i] if b == 2 else kind_recv.at[g, i // CUTS],
            device_id=seq_dev(d), device_id_type=MESH)

    def slots(g, ref, sem):
        return pltpu.make_async_remote_copy(
            src_ref=ref, dst_ref=ref, send_sem=sem, recv_sem=sem,
            device_id=sibling, device_id_type=MESH)

    def got(g, kind):
        slots(g, kv.at[g, 0:2, kind], kind_recv.at[g, kind]).wait_recv()

    def send_own(g):
        for i in range(PIECES):
            kv_copy(g, i, 2, 0, 2, True).start()

            @pl.when(odd == 0)
            def _():
                kv_copy(g, i, 1, 0, 1, True).start()

    def relay_two(g):
        for i in range(PIECES):
            kv_copy(g, i, 2, 0, 2).wait_recv()

            @pl.when(odd == 1)
            def _():
                kv_copy(g, i, 1, 2, -1).start()
                kv_copy(g, i, 3, 2, 1).start()

            @pl.when(odd == 0)
            def _():
                kv_copy(g, i, 3, 2, 1).start()

    def own_sent(g):
        for parity, count in ((0, 2), (1, 1)):
            @pl.when(odd == parity)
            def _():
                slots(g, kv.at[g, 0:count], own_send.at[g]).wait_send()

    def relays_sent(g):
        for parity, count in ((0, 1), (1, 2)):
            @pl.when(odd == parity)
            def _():
                slots(g, kv.at[g, 0:count], relay_send.at[g]).wait_send()

    def keys_lent():
        return pltpu.make_async_remote_copy(
            src_ref=kv.at[last, 0], dst_ref=kv.at[groups, 0],
            send_sem=lend_send.at[0], recv_sem=lend_recv.at[0],
            device_id=match, device_id_type=MESH)

    def queries_lent(m, first):
        return pltpu.make_async_remote_copy(
            src_ref=qv.at[:, pl.ds(first * HEAD, m * HEAD)], dst_ref=qx.at[:, pl.ds(0, m * HEAD)],
            send_sem=lend_send.at[1], recv_sem=lend_recv.at[1],
            device_id=match, device_id_type=MESH)

    def loaded(g):
        pltpu.make_async_copy(kv.at[g, 1], kv.at[g, 0], ld_sem.at[min(g, 1)]).wait()

    loaded(0)

    @on_core(1)
    def _():
        send_own(0)

    if groups > 1:
        ref = kv.at[1:groups, 0]
        pltpu.make_async_copy(ref, ref, ld_sem.at[1]).wait()
    q_load.wait()

    def lend(m, first):
        keys_lent().start()
        queries_lent(m, first).start()

    lenders(lend)

    @on_core(1)
    def _():
        own_sent(0)
        pl.semaphore_signal(go_sem, inc=1, device_id=sibling, device_id_type=MESH)

    @on_core(0)
    def _():
        pl.semaphore_wait(go_sem, 1)
        send_own(0)

    bp_load.wait()
    blk = half
    lane = lax.broadcasted_iota(jnp.int32, (blk, blk), 1)
    sub = lax.broadcasted_iota(jnp.int32, (blk, blk), 0)
    for i in range(2):
        qpos = bp[2 * s + i] * blk + sub
        for b in range(WINDOW):
            owner = lax.rem(s - b + n, n)
            for j in range(2):
                kpos = bp[2 * owner + j] * blk + lane
                bias[i * blk:(i + 1) * blk, (2 * b + j) * blk:(2 * b + j + 1) * blk] = (
                    jnp.where(kpos <= qpos, 0.0, -1e30).astype(jnp.float32))

    relay_two(0)
    for g in range(1, groups):
        send_own(g)

    def pass_on(m, first):
        keys_lent().wait_recv()
        send_own(groups)

    borrowers(pass_on)

    def piece(owner, h, count=1):
        col = pl.multiple_of((owner * heads + h) * HEAD, HEAD)
        return out.at[:, pl.ds(col, count * HEAD)]

    def x_copy(k, h, owner, count=1):
        return pltpu.make_async_remote_copy(
            src_ref=piece(owner, h, count), dst_ref=piece(owner, h, count),
            send_sem=x_send.at[k - 1], recv_sem=x_recv.at[k - 1, h // 2],
            device_id=x_dev(k), device_id_type=MESH)

    def c_copy(k, h, owner, count=1):
        return pltpu.make_async_remote_copy(
            src_ref=piece(owner, h, count), dst_ref=piece(owner, h, count),
            send_sem=c_send.at[k], recv_sem=c_recv.at[k],
            device_id=sibling, device_id_type=MESH)

    factor = math.log2(math.e) / math.sqrt(HEAD)
    window = WINDOW * rows

    def attend(g, jobs, late=None):
        keys = kv[g, :, 0].reshape(window, HEAD)
        made = []
        for queries, qcol, col in jobs:
            qcol = pl.multiple_of(qcol, HEAD)
            col = pl.multiple_of(col, HEAD)
            for i in range(2):
                part = slice(i * half, (i + 1) * half)
                q = queries[part, pl.ds(qcol, HEAD)]
                sc = lax.dot_general(q, keys, (((1,), (1,)), ((), ())),
                                     preferred_element_type=jnp.float32)
                sc = sc + bias[part, :]
                top = jnp.max(sc, axis=1, keepdims=True)
                w = jnp.exp2((sc - top) * factor)
                total = jnp.sum(w, axis=1, keepdims=True)
                made.append((part, col, w.astype(jnp.bfloat16), total))
        if late is not None:
            late()
        vals = kv[g, :, 1].reshape(window, HEAD)
        for part, col, w, total in made:
            mixed = jnp.dot(w, vals, preferred_element_type=jnp.float32)
            out[part, pl.ds(col, HEAD)] = (mixed / total).astype(out.dtype)

    def own_heads(g, first, count, late=None):
        attend(g, [(qv, h * HEAD, (t * heads + h) * HEAD) for h in range(first, first + count)], late)
        for h in range(first, first + count, 2):
            for c in range(2):
                if h < keep[c]:
                    @on_core(c)
                    def _():
                        for k in range(1, hops + 1):
                            x_copy(k, h, t, 2).start()
        c_copy(0, first, t, count).start()

    def lent_heads(r, _, step, first):
        r = r * step
        attend(groups, [(qx, (r + j) * HEAD, (other * heads + first + r + j) * HEAD) for j in range(step)])
        c_copy(hops + 1, first + r, other, step).start()
        return 0

    def forward(h, _):
        h = 2 * h
        for k in range(1, hops + 1):
            owner = lax.rem(t - 2 * k + T, T)
            x_copy(k, h, owner, 2).wait_recv()
            c_copy(k, h, owner, 2).start()
        return 0

    def relay(g, f):
        if g < groups:
            f(g)
        elif g < every:
            borrowers(lambda m, first: f(g))

    def arrive(g):
        got(g, 0)
        got(g, 1)

    for g in range(groups):
        base = g * GROUP
        if g == 0:
            got(0, 0)
            own_heads(0, 0, 2, lambda: got(0, 1))
            own_heads(0, 2, 2)
            relay(1, relay_two)
        else:
            relay(g + 1, relay_two)
            arrive(g)
            own_heads(g, base, 4)
        own_heads(g, base + 4, 4)

    def forwards(first, end):
        lax.fori_loop(first // 2, end // 2, forward, 0)

    done = [0, 0]

    def borrowed(m, first):
        c = 1 - share.index(m)
        stops = [min(x, keep[c]) for x in AHEAD]
        forwards(0, stops[0])
        arrive(groups)
        queries_lent(m, first).wait_recv()
        step = math.gcd(m, 4)
        for r in range(m // step):
            lent_heads(r, 0, step, first)
            if r == 0:
                forwards(stops[0], stops[1])
        done[c] = stops[1]

    borrowers(borrowed)
    for c in range(2):
        @on_core(c)
        def _():
            forwards(done[c], keep[c])

    for g in range(groups):
        relays_sent(g)
        if g > 0:
            own_sent(g)
    on_core(0)(lambda: own_sent(0))

    def settle(m, first):
        relays_sent(groups)
        own_sent(groups)
        c_copy(hops + 1, first, other, m).wait_send()

    borrowers(settle)

    def settle_lent(m, first):
        keys_lent().wait_send()
        queries_lent(m, first).wait_send()
        c_copy(hops + 1, first, t, m).wait_recv()

    lenders(settle_lent)
    c_copy(0, 0, t, heads).wait()

    for c in range(2):
        @on_core(c)
        def _():
            for k in range(1, hops + 1):
                x_copy(k, 0, t, keep[c]).wait_send()
                c_copy(k, 0, t, keep[c]).wait_send()
                c_copy(k, 0, t, keep[1 - c]).wait_recv()


def body(n, T, queries, keys, values, block_pos):
    rows = queries.shape[0]
    groups = keys.shape[1] // HEAD
    heads = groups * GROUP
    hops = T // 2 - 1
    share = SHARE if hops == 1 and groups > 1 else (0, 0)
    every = groups + (1 if any(share) else 0)
    dma = pltpu.SemaphoreType.DMA
    return pl.pallas_call(
        functools.partial(kernel, n, T, rows, groups, share),
        out_shape=jax.ShapeDtypeStruct((rows, queries.shape[1] * T), jnp.bfloat16),
        in_specs=[pl.BlockSpec(memory_space=pltpu.HBM)] * 4,
        out_specs=pl.BlockSpec(memory_space=pltpu.VMEM),
        scratch_shapes=[
            pltpu.SMEM(block_pos.shape, jnp.int32),
            pltpu.VMEM((rows, heads * HEAD), jnp.bfloat16),
            pltpu.VMEM((rows, max(*share, 1) * HEAD), jnp.bfloat16),
            pltpu.VMEM((every, WINDOW, 2, rows, HEAD), jnp.bfloat16),
            pltpu.VMEM((rows, WINDOW * rows), jnp.float32),
            dma((4,)),
            pltpu.SemaphoreType.REGULAR,
            dma((every,)),
            dma((every,)),
            dma((every, PIECES)),
            dma((every, 2)),
            dma((2,)),
            dma((2,)),
            dma((hops,)),
            dma((hops, heads // 2)),
            dma((hops + 2,)),
            dma((hops + 2,)),
        ],
        compiler_params=pltpu.CompilerParams(
            collective_id=0, has_side_effects=True, vmem_limit_bytes=32 * 1024 * 1024),
    )(*(pltpu.with_memory_space_constraint(z, pltpu.HBM)
        for z in (queries, keys, values, block_pos)))


def solution(mesh):
    n, T = mesh.shape["seq"], mesh.shape["tensor"]
    placed = (P("seq", "tensor"), P("seq", "tensor"), P("seq", "tensor"), P())
    return jax.shard_map(functools.partial(body, n, T), mesh=mesh, in_specs=placed,
                         out_specs=P("seq", None), check_vma=False)
```
